32 devices in a mesh: seq: 16 (over z, x, core), head: 2 (over y).
Axes of the slice: x: 2, y: 2, z: 4, core: 2. Of those that a mesh axis runs over, the one named last changes fastest.
Arguments:
- activations: bfloat16 [4096, 4096], P('seq', 'head'), may hold values from -6 to 6
- grad_out: bfloat16 [4096, 4096], P('seq', 'head'), may hold values from -0.03125 to 0.03125
- query_weight: bfloat16 [4096, 4096], P('seq', 'head'), may hold values from -0.09375 to 0.09375
- key_weight: bfloat16 [4096, 1024], P('seq', 'head'), may hold values from -0.09375 to 0.09375
- value_weight: bfloat16 [4096, 1024], P('seq', 'head'), may hold values from -0.09375 to 0.09375
Outputs:
- grad_input: bfloat16 [4096, 4096], P('seq', 'head')
The draws below stay inside these ranges and needn't reach their ends.
All inputs are finite; a program needn't handle non-finite values.
Results may differ from the reference program's by a relative error of at most 0.018.
Values may be sent and summed in bfloat16 or wider, within the bound.
No kernel may reach another device: no remote copies, remote signals or barrier semaphores. Data moves between devices by JAX's collectives and lax.ppermute only.
A program may use at most 128 MiB of HBM per device.

```python
import jax
import jax.numpy as jnp
from jax import lax

D = 4096
HEADS = 32
KV_HEADS = 8
HEAD_DIM = 128
TOK_DEV = 256
TOKENS = 4096


def shard_levels(rng, dims, shards, low, top_value):
    gain, own = 1.0, jax.random.fold_in(rng, 6)
    for axis_at, shards_of in shards:
        heights = jnp.exp(jax.random.uniform(jax.random.fold_in(own, axis_at), (shards_of,), jnp.float32, low / len(shards), top_value / len(shards)))
        gain = gain * jnp.repeat(heights, dims[axis_at] // shards_of).reshape([-1 if axis == axis_at else 1 for axis in range(len(dims))])
    return gain


def noise(stream_key, shape, width, most, pieces=(), dtype=jnp.bfloat16):
    array = width * jax.random.normal(stream_key, shape, jnp.float32)
    if pieces:
        array = array * shard_levels(stream_key, shape, pieces, -0.22, 0.18)
    return jnp.clip(array, -most, most).astype(dtype)


def setup_inputs(seed: int = 0) -> dict:
    key_list = jax.random.split(jax.random.key(seed), 6)
    activations = noise(key_list[0], (TOKENS, D), 1.0, 6.0, ((0, 16), (1, 2)))
    grad_out = noise(key_list[1], (TOKENS, HEADS * HEAD_DIM), 0.005, 0.03125, ((0, 16), (1, 2)))
    query_weight = noise(key_list[2], (D, HEADS * HEAD_DIM), D ** -0.5, 0.09375, ((0, 16), (1, 2)))
    key_weight = noise(key_list[3], (D, KV_HEADS * HEAD_DIM), D ** -0.5, 0.09375, ((0, 16), (1, 2)))
    value_weight = noise(key_list[4], (D, KV_HEADS * HEAD_DIM), D ** -0.5, 0.09375, ((0, 16), (1, 2)))
    return dict(activations=activations, grad_out=grad_out, query_weight=query_weight, key_weight=key_weight, value_weight=value_weight)


def reference(activations, grad_out, query_weight, key_weight, value_weight):
    factor = HEAD_DIM ** -0.5
    group_size = HEADS // KV_HEADS
    shard_count = TOKENS // TOK_DEV
    queries = jnp.dot(activations, query_weight, preferred_element_type=jnp.float32).astype(jnp.bfloat16)
    key_rows = jnp.dot(activations, key_weight, preferred_element_type=jnp.float32).astype(jnp.bfloat16)
    value_rows = jnp.dot(activations, value_weight, preferred_element_type=jnp.float32).astype(jnp.bfloat16)
    queries, key_rows, value_rows = lax.optimization_barrier((queries, key_rows, value_rows))
    query_heads = queries.reshape(shard_count, TOK_DEV, KV_HEADS, group_size, HEAD_DIM)
    key_heads = key_rows.reshape(shard_count, TOK_DEV, KV_HEADS, HEAD_DIM)
    value_heads = value_rows.reshape(shard_count, TOK_DEV, KV_HEADS, HEAD_DIM)
    grad_heads = grad_out.reshape(shard_count, TOK_DEV, KV_HEADS, group_size, HEAD_DIM)
    kv_state = jnp.einsum('ntgd,ntge->ngde', key_heads.astype(jnp.float32), value_heads.astype(jnp.float32)).astype(jnp.bfloat16)
    grad_state = (factor * jnp.einsum('ntghd,ntghe->ngde', query_heads.astype(jnp.float32), grad_heads.astype(jnp.float32))).astype(jnp.bfloat16)
    kv_state, grad_state = lax.optimization_barrier((kv_state, grad_state))
    kv_wide = kv_state.astype(jnp.float32)
    grad_wide = grad_state.astype(jnp.float32)
    running = jnp.cumsum(kv_wide, axis=0)
    prefix = jnp.concatenate([jnp.zeros_like(running[:1]), running[:-1]], axis=0)
    behind = jnp.cumsum(grad_wide[::-1], axis=0)[::-1]
    suffix = jnp.concatenate([behind[1:], jnp.zeros_like(behind[:1])], axis=0)
    prefix_half, suffix_half = lax.optimization_barrier((prefix.astype(jnp.bfloat16), suffix.astype(jnp.bfloat16)))
    causal = jnp.arange(TOK_DEV)[:, None] >= jnp.arange(TOK_DEV)[None, :]

    def one_shard(items):
        query_blk, key_blk, value_blk, grad_blk, prefix_blk, suffix_blk = items
        query_wide = query_blk.astype(jnp.float32)
        key_wide = key_blk.astype(jnp.float32)
        value_wide = value_blk.astype(jnp.float32)
        grad_wide_blk = grad_blk.astype(jnp.float32)
        prefix_wide = prefix_blk.astype(jnp.float32)
        suffix_wide = suffix_blk.astype(jnp.float32)
        scores = jnp.where(causal, jnp.einsum('tghd,sgd->ghts', query_wide, key_wide), 0.0).astype(jnp.bfloat16)
        grad_scores = jnp.where(causal, jnp.einsum('tghe,sge->ghts', grad_wide_blk, value_wide), 0.0).astype(jnp.bfloat16)
        scores, grad_scores = lax.optimization_barrier((scores, grad_scores))
        scores_wide = scores.astype(jnp.float32)
        grad_scores_wide = grad_scores.astype(jnp.float32)
        grad_query = factor * (jnp.einsum('ghts,sgd->tghd', grad_scores_wide, key_wide) + jnp.einsum('tghe,gde->tghd', grad_wide_blk, prefix_wide))
        grad_key = factor * jnp.einsum('ghts,tghd->sgd', grad_scores_wide, query_wide) + jnp.einsum('sge,gde->sgd', value_wide, suffix_wide)
        grad_value = factor * jnp.einsum('ghts,tghe->sge', scores_wide, grad_wide_blk) + jnp.einsum('sgd,gde->sge', key_wide, suffix_wide)
        return (grad_query.astype(jnp.bfloat16).reshape(TOK_DEV, -1),
                grad_key.astype(jnp.bfloat16).reshape(TOK_DEV, -1),
                grad_value.astype(jnp.bfloat16).reshape(TOK_DEV, -1))

    grad_query, grad_key, grad_value = lax.map(one_shard, (query_heads, key_heads, value_heads, grad_heads, prefix_half, suffix_half))
    grad_query = grad_query.reshape(TOKENS, -1)
    grad_key = grad_key.reshape(TOKENS, -1)
    grad_value = grad_value.reshape(TOKENS, -1)
    total = jnp.dot(grad_query, query_weight.T, preferred_element_type=jnp.float32)
    total = total + jnp.dot(grad_key, key_weight.T, preferred_element_type=jnp.float32)
    total = total + jnp.dot(grad_value, value_weight.T, preferred_element_type=jnp.float32)
    return total.astype(jnp.bfloat16)
```

```python
import jax
import jax.numpy as jnp
from jax import lax
from jax.experimental import pallas as pl
from jax.experimental.pallas import tpu as pltpu
from jax.sharding import PartitionSpec as P


HEADS = 32
KV_HEADS = 8
HEAD_DIM = 128
GROUP = HEADS // KV_HEADS
FACTOR = HEAD_DIM ** (-0.5)
F32 = jnp.float32
BF16 = jnp.bfloat16


def dot_nt(a, b):
    return lax.dot_general(a, b, (((1,), (1,)), ((), ())), preferred_element_type=F32)


def make_plain():
    def local(activations, grad_out, query_weight, key_weight, value_weight):
        gathered = tuple(
            lax.all_gather(w, "seq", axis=0, tiled=True)
            for w in (query_weight, key_weight, value_weight)
        )
        tokens = activations.shape[0]
        whole = lax.all_gather(activations, "head", axis=1, tiled=True)
        queries, keys, values = (
            jnp.dot(whole, w, preferred_element_type=F32).astype(BF16) for w in gathered
        )
        groups = keys.shape[1] // HEAD_DIM
        q = queries.reshape(tokens, groups, GROUP, HEAD_DIM)
        k = keys.reshape(tokens, groups, HEAD_DIM)
        v = values.reshape(tokens, groups, HEAD_DIM)
        do = grad_out.reshape(tokens, groups, GROUP, HEAD_DIM)
        kv_state = jnp.einsum("tgd,tge->gde", k, v, preferred_element_type=F32).astype(BF16)
        grad_state = (
            FACTOR * jnp.einsum("tghd,tghe->gde", q, do, preferred_element_type=F32)
        ).astype(BF16)
        every_kv = lax.all_gather(kv_state[None], "seq", axis=0, tiled=True)
        every_grad = lax.all_gather(grad_state[None], "seq", axis=0, tiled=True)
        position = lax.axis_index("seq")
        order = jnp.arange(every_kv.shape[0], dtype=jnp.int32)
        before = (order < position).astype(BF16)
        after = (order > position).astype(BF16)
        prefix = jnp.einsum("n,ngde->gde", before, every_kv, preferred_element_type=F32).astype(BF16)
        suffix = jnp.einsum("n,ngde->gde", after, every_grad, preferred_element_type=F32).astype(BF16)
        causal = jnp.arange(tokens)[:, None] >= jnp.arange(tokens)[None, :]
        s = jnp.where(
            causal, jnp.einsum("tghd,sgd->ghts", q, k, preferred_element_type=F32), 0.0
        ).astype(BF16)
        ds = jnp.where(
            causal, jnp.einsum("tghe,sge->ghts", do, v, preferred_element_type=F32), 0.0
        ).astype(BF16)
        grad_query = FACTOR * (
            jnp.einsum("ghts,sgd->tghd", ds, k, preferred_element_type=F32)
            + jnp.einsum("tghe,gde->tghd", do, prefix, preferred_element_type=F32)
        )
        grad_key = FACTOR * jnp.einsum(
            "ghts,tghd->sgd", ds, q, preferred_element_type=F32
        ) + jnp.einsum("sge,gde->sgd", v, suffix, preferred_element_type=F32)
        grad_value = FACTOR * jnp.einsum(
            "ghts,tghe->sge", s, do, preferred_element_type=F32
        ) + jnp.einsum("sgd,gde->sge", k, suffix, preferred_element_type=F32)
        parts = (
            dot_nt(g.astype(BF16).reshape(tokens, -1), w)
            for g, w in zip((grad_query, grad_key, grad_value), gathered)
        )
        return lax.psum_scatter(
            sum(parts).astype(BF16), "head", scatter_dimension=1, tiled=True
        )

    return local


def mm(a, b, contract):
    return lax.dot_general(a, b, (contract, ((), ())), preferred_element_type=F32)


NN, NT, TN = ((1,), (0,)), ((1,), (1,)), ((0,), (0,))


def causal_mask(n):
    return lax.broadcasted_iota(jnp.int32, (n, n), 0) >= lax.broadcasted_iota(
        jnp.int32, (n, n), 1
    )


def head_cols(h):
    return slice(h * HEAD_DIM, (h + 1) * HEAD_DIM)


def state_kernel(kv_ref, out_ref, total_ref):
    tokens = kv_ref.shape[0] // 2
    for g in range(out_ref.shape[1]):
        total = jnp.zeros(total_ref.shape[1:], F32)
        for n in range(out_ref.shape[0]):
            t = slice(n * tokens, (n + 1) * tokens)
            k, v = kv_ref[t, head_cols(2 * g)], kv_ref[t, head_cols(2 * g + 1)]
            state = mm(k, v, TN).astype(BF16)
            out_ref[n, g] = state
            total = total + state.astype(F32)
        total_ref[g] = total.astype(BF16)


def grad_query_kernel(k_ref, v_ref, do_ref, prefix_ref, out_ref):
    k, v, prefix = k_ref[...], v_ref[...], prefix_ref[0, 0]
    mask = causal_mask(k.shape[0])
    for h in range(GROUP):
        do = do_ref[:, head_cols(h)]
        ds = jnp.where(mask, mm(do, v, NT), 0.0).astype(BF16)
        out_ref[:, head_cols(h)] = (FACTOR * (mm(ds, k, NN) + mm(do, prefix, NT))).astype(BF16)


def inner_kernel(q_ref, k_ref, v_ref, do_ref, out_ref):
    k, v = k_ref[...], v_ref[...]
    shape = (k.shape[0], k.shape[0])
    mask = lax.broadcasted_iota(jnp.int32, shape, 0) <= lax.broadcasted_iota(jnp.int32, shape, 1)
    gk = jnp.zeros(k.shape, F32)
    gv = jnp.zeros(k.shape, F32)
    for h in range(GROUP):
        q, do = q_ref[:, head_cols(h)], do_ref[:, head_cols(h)]
        ds = jnp.where(mask, mm(v, do, NT), 0.0).astype(BF16)
        s = jnp.where(mask, mm(k, q, NT), 0.0).astype(BF16)
        gk = gk + mm(ds, q, NN)
        gv = gv + mm(s, do, NN)
    out_ref[:, head_cols(0)] = FACTOR * gk
    out_ref[:, head_cols(1)] = FACTOR * gv


def outer_kernel(flag_ref, kv_ref, outside_ref, got_ref, state_ref, *refs):
    inner_refs, out_refs = refs[:-2], refs[-2:]
    tokens = kv_ref.shape[0] // 2
    for g, inner_ref in enumerate(inner_refs):
        behind = outside_ref[g] + jnp.where(flag_ref[0] == 1, got_ref[g].astype(F32), 0.0)
        for n in range(2):
            add = (flag_ref[1] == 1) if n == 0 else (flag_ref[1] == 0)
            suffix = behind + jnp.where(add, state_ref[1 - n, g].astype(F32), 0.0)
            suffix = suffix.astype(BF16)
            t = slice(n * tokens, (n + 1) * tokens)
            k, v = kv_ref[t, head_cols(2 * g)], kv_ref[t, head_cols(2 * g + 1)]
            gk = inner_ref[t, head_cols(0)] + mm(v, suffix, NT)
            gv = inner_ref[t, head_cols(1)] + mm(k, suffix, NN)
            out_refs[n][:, head_cols(2 * g)] = gk.astype(BF16)
            out_refs[n][:, head_cols(2 * g + 1)] = gv.astype(BF16)


def project_call(base, x, weights, total, dtype, do=None):
    slots = sorted(weights)
    rows, cols = weights[slots[0]].shape
    tokens = x.shape[0] // 2
    width = GROUP * HEAD_DIM if do is not None else rows // 2
    n = len(slots)

    def body(base_ref, *refs):
        xs, ws = refs[:n], refs[n : 2 * n]
        rest = list(refs[2 * n :])
        acc = rest.pop(0)[...] if total is not None else None
        do_ref = rest.pop(0) if do is not None else None
        for x_ref, w_ref in zip(xs, ws):
            part = mm(x_ref[...], w_ref[...], NN)
            acc = part if acc is None else acc + part
        acc = acc.astype(dtype)
        rest[0][...] = acc
        if do_ref is not None:
            both = None
            for m in range(2):
                t = slice(m * tokens, (m + 1) * tokens)
                state = None
                for h in range(GROUP):
                    part = mm(acc[t, head_cols(h)], do_ref[t, head_cols(h)], TN)
                    state = part if state is None else state + part
                state = (FACTOR * state).astype(BF16)
                rest[1][m, 0] = state
                state = state.astype(F32)
                both = state if both is None else both + state
            rest[2][0] = both.astype(BF16)

    def x_spec(i):
        return pl.BlockSpec((2 * tokens, rows), lambda j, b: (0, b[0] ^ i))

    tile = pl.BlockSpec((2 * tokens, width), lambda j, b: (0, j))
    args = [x] * n + [weights[i] for i in slots]
    in_specs = [x_spec(i) for i in slots]
    in_specs += [pl.BlockSpec((rows, width), lambda j, b: (0, j))] * n
    out_shape, out_specs = [jax.ShapeDtypeStruct((2 * tokens, cols), dtype)], [tile]
    if total is not None:
        args.append(total)
        in_specs.append(tile)
    if do is not None:
        args.append(do)
        in_specs.append(tile)
        one = (cols // width, HEAD_DIM, HEAD_DIM)
        out_shape += [jax.ShapeDtypeStruct((2,) + one, BF16), jax.ShapeDtypeStruct(one, BF16)]
        out_specs += [
            pl.BlockSpec((2, 1, HEAD_DIM, HEAD_DIM), lambda j, b: (0, j, 0, 0)),
            pl.BlockSpec((1, HEAD_DIM, HEAD_DIM), lambda j, b: (j, 0, 0)),
        ]
    out = pl.pallas_call(
        body,
        out_shape=out_shape,
        grid_spec=pltpu.PrefetchScalarGridSpec(
            num_scalar_prefetch=1,
            grid=(cols // width,),
            in_specs=in_specs,
            out_specs=out_specs,
        ),
    )(base, *args)
    return out if do is not None else out[0]


def back_call(side, grads, low, high):
    weights = low + high
    n = len(low)
    rows, inner = weights[0].shape
    tokens = grads.shape[0] // 2
    half = rows // 2

    def body(side_ref, g_ref, *refs):
        ws, (keep_ref, send_ref) = refs[:-2], refs[-2:]
        for m, w_ref in enumerate(ws):

            @pl.when(pl.program_id(0) == m)
            def _():
                both = mm(g_ref[...], w_ref[...], NT)
                keep_ref[0] = both[:tokens]
                send_ref[0] = both[tokens:].astype(BF16)

    def w_spec(m):
        return pl.BlockSpec(
            (half, inner),
            lambda i, j, b: (jnp.where(i == m, j, jnp.where(i < m, 0, 1)), 0),
        )

    out = pl.BlockSpec(
        (1, tokens, half), lambda i, j, b: ((i // n) ^ b[0], 0, (i % n) * 2 + j)
    )
    shape = (2, tokens, n * rows)
    return pl.pallas_call(
        body,
        out_shape=(jax.ShapeDtypeStruct(shape, F32), jax.ShapeDtypeStruct(shape, BF16)),
        grid_spec=pltpu.PrefetchScalarGridSpec(
            num_scalar_prefetch=1,
            grid=(2 * n, 2),
            in_specs=[pl.BlockSpec(grads.shape, lambda i, j, b: (0, 0))]
            + [w_spec(m) for m in range(2 * n)],
            out_specs=(out, out),
        ),
    )(side, grads, *weights)


def finish_kernel(base_ref, sum_ref, g_ref, w_ref, w_other_ref, out_ref):
    n = w_ref.shape[1]
    total = sum_ref[...] + mm(g_ref[:, :n], w_ref[...], NT)
    out_ref[...] = (total + mm(g_ref[:, n:], w_other_ref[...], NT)).astype(BF16)


def make_split(zs, xs, ys):
    n_seq = zs * xs * 2

    def swap(value, bit):
        return lax.ppermute(value, "seq", [(s, s ^ bit) for s in range(n_seq)])

    def swap_y(value):
        return lax.ppermute(value, "head", [(y, y ^ 1) for y in range(ys)])

    Z1, Z2, X1, C1 = 2 * xs, 4 * xs, 2, 1

    def local(activations, grad_out, query_weight, key_weight, value_weight):
        tokens, _ = activations.shape
        groups = key_weight.shape[1] // HEAD_DIM // 2
        seq = lax.axis_index("seq")
        y = lax.axis_index("head")
        core, x, z = seq % 2, (seq // 2) % xs, seq // (2 * xs)
        chip, chips = seq // 2, n_seq // 2
        per_half = chips // ys
        side = (chip // per_half) ^ y

        def cols(w, which):
            n = w.shape[1] // 2
            return lax.dynamic_slice_in_dim(w, which * n, n, 1)

        def own_and_other(own, other):
            return jnp.concatenate([own, swap(other, C1)], 0)

        def in_order(own, other):
            n = own.shape[0]
            both = jnp.zeros((2 * n, own.shape[1]), own.dtype)
            both = lax.dynamic_update_slice_in_dim(both, own, core * n, 0)
            got = swap(other, C1)
            return lax.dynamic_update_slice_in_dim(both, got, (1 - core) * n, 0)

        def keys_and_values(which):
            k, v = cols(key_weight, which), cols(value_weight, which)
            return jnp.concatenate(
                [w[:, head_cols(g)] for g in range(groups) for w in (k, v)], 1
            )

        def scalar(value):
            return value.reshape(1).astype(jnp.int32)

        chunk_a = in_order(keys_and_values(core), keys_and_values(1 - core))
        chunk_b = in_order(cols(query_weight, core), cols(query_weight, 1 - core))
        do_all = own_and_other(cols(grad_out, core), cols(grad_out, 1 - core))
        acts = jnp.concatenate([activations, swap_y(activations)], 1)
        acts = own_and_other(acts, acts)
        base = scalar(side * per_half + chip % per_half)

        def project(weights, which, total, dtype, do=None):
            return project_call(
                base, acts, {i: weights[i] for i in which}, total, dtype, do
            )

        w_kv, w_q = [chunk_a] + [None] * (chips - 1), [chunk_b] + [None] * (chips - 1)
        w_kv[4], w_kv[2] = swap(chunk_a, Z2), swap(chunk_a, Z1)
        w_kv[1], w_q[1] = swap(chunk_a, X1), swap(chunk_b, X1)
        w_kv[6] = swap(w_kv[4], Z1)
        w_q[4], w_q[2] = swap(chunk_b, Z2), swap(chunk_b, Z1)
        w_kv[3], w_kv[5] = swap(w_kv[2], X1), swap(w_kv[4], X1)
        w_kv[7] = swap(w_kv[6], X1)
        kv_sum = project(w_kv, (0, 1, 2, 4), None, F32)
        w_q[5], w_q[6] = swap(w_q[4], X1), swap(w_q[4], Z1)
        kv = project(w_kv, (3, 5, 6, 7), kv_sum, BF16)
        w_q[3] = swap(w_q[2], X1)
        q_sum = project(w_q, (0, 1, 2, 4), None, F32)
        cut = chunk_b.shape[0] * 3 // 8
        w_q[7] = jnp.concatenate([swap(w_q[6][:cut], X1), swap(w_q[5][cut:], Z1)], 0)

        n_half = chips // ys
        low, high = jnp.concatenate(w_kv[:n_half], 0), jnp.concatenate(w_kv[n_half:], 0)
        w_home = jnp.where(side == 0, low, high)
        w_home_y = swap_y(jnp.where(side == 0, high, low))
        w_home_c = swap(w_home, C1)
        w_home_cy = swap(w_home_y, C1)

        n_cols = GROUP * HEAD_DIM
        states = jax.ShapeDtypeStruct((2, groups, HEAD_DIM, HEAD_DIM), BF16)

        def scan(total, ahead):
            total = total.astype(F32)
            outside = jnp.zeros_like(total)
            for bit, at in ((X1, x), (Z1, z % 2), (Z2, z // 2)):
                got = swap(total.astype(BF16), bit)
                counts = (at == 1) == ahead
                if bit == Z2:
                    return outside, got, counts
                outside = outside + jnp.where(counts, got.astype(F32), 0.0)
                total = total + got.astype(F32)

        totals = jax.ShapeDtypeStruct(states.shape[1:], BF16)
        state, total = pl.pallas_call(state_kernel, out_shape=(states, totals))(kv)
        outside, got, counts = scan(total, True)
        outside = outside + jnp.where(counts, got.astype(F32), 0.0)
        prefix = jnp.stack(
            [
                outside + jnp.where(core == 1, state[1].astype(F32), 0.0),
                outside + jnp.where(core == 0, state[0].astype(F32), 0.0),
            ]
        ).astype(BF16)
        q_spec = pl.BlockSpec((tokens, n_cols), lambda n, g: (n, g))
        gq = pl.pallas_call(
            grad_query_kernel,
            out_shape=jax.ShapeDtypeStruct((2 * tokens, groups * n_cols), BF16),
            grid=(2, groups),
            in_specs=[
                pl.BlockSpec((tokens, HEAD_DIM), lambda n, g: (n, 2 * g)),
                pl.BlockSpec((tokens, HEAD_DIM), lambda n, g: (n, 2 * g + 1)),
                q_spec,
                pl.BlockSpec((1, 1, HEAD_DIM, HEAD_DIM), lambda n, g: (n, g, 0, 0)),
            ],
            out_specs=q_spec,
        )(kv, kv, do_all, prefix)

        def back(which):
            keep, send = back_call(
                scalar(side), gq, [w_q[i] for i in which], [w_q[i + n_half] for i in which]
            )
            got = swap(send, C1)
            away = (keep[1] + got[1].astype(F32)).astype(BF16)
            return keep[0], got[0], swap_y(away)

        early = back(range(n_half - 1))
        q_sum = project(w_q, (5, 6), q_sum, F32)
        q, gs, total = project(w_q, (3, 7), q_sum, BF16, do_all)
        outside, got, counts = scan(total, False)
        inner = []
        for g in range(groups):
            inner.append(
                pl.pallas_call(
                    inner_kernel,
                    out_shape=jax.ShapeDtypeStruct((2 * tokens, 2 * HEAD_DIM), F32),
                    grid=(2,),
                    in_specs=[
                        pl.BlockSpec((tokens, n_cols), lambda n, g=g: (n, g)),
                        pl.BlockSpec((tokens, HEAD_DIM), lambda n, g=g: (n, 2 * g)),
                        pl.BlockSpec((tokens, HEAD_DIM), lambda n, g=g: (n, 2 * g + 1)),
                        pl.BlockSpec((tokens, n_cols), lambda n, g=g: (n, g)),
                    ],
                    out_specs=pl.BlockSpec((tokens, 2 * HEAD_DIM), lambda n: (n, 0)),
                )(q, kv, kv, do_all)
            )
        late = back((n_half - 1,))
        flags = jnp.stack([counts, core == 0]).astype(jnp.int32)
        part = jax.ShapeDtypeStruct((tokens, 2 * groups * HEAD_DIM), BF16)
        vmem = pl.BlockSpec(memory_space=pltpu.VMEM)
        gkv, gkv_other = pl.pallas_call(
            outer_kernel,
            out_shape=(part, part),
            in_specs=[pl.BlockSpec(memory_space=pltpu.SMEM)] + [vmem] * (4 + groups),
            out_specs=(vmem, vmem),
        )(flags, kv, outside, got, gs, *inner)
        gkv_c = swap(gkv_other, C1)
        far = swap_y(jnp.concatenate([gkv, gkv_c], 1))
        home = jnp.concatenate(
            [p[0] + p[1].astype(F32) + p[2].astype(F32) for p in (early, late)], 1
        )
        home = home + mm(gkv, w_home, NT) + mm(gkv_c, w_home_c, NT)
        width = home.shape[1] // n_half
        w_spec = pl.BlockSpec((width, w_home.shape[1]), lambda i, b: (b[0] ^ i, 0))
        return pl.pallas_call(
            finish_kernel,
            out_shape=jax.ShapeDtypeStruct(home.shape, BF16),
            grid_spec=pltpu.PrefetchScalarGridSpec(
                num_scalar_prefetch=1,
                grid=(n_half,),
                in_specs=[
                    pl.BlockSpec((tokens, width), lambda i, b: (0, b[0] ^ i)),
                    pl.BlockSpec(far.shape, lambda i, b: (0, 0)),
                    w_spec,
                    w_spec,
                ],
                out_specs=pl.BlockSpec((tokens, width), lambda i, b: (0, i)),
            ),
        )(scalar(chip % per_half), home, far, w_home_y, w_home_cy)

    return local


def solution(mesh):
    n_seq, n_head = mesh.shape["seq"], mesh.shape["head"]
    groups = KV_HEADS // n_head
    split = n_seq == 4 * 2 * 2 and groups % 2 == 0 and n_head == 2
    local = make_split(n_seq // 4, 2, n_head) if split else make_plain()

    spec = P("seq", "head")
    return jax.shard_map(local, mesh=mesh, in_specs=(spec,) * 5, out_specs=spec, check_vma=False)
```

```python
import jax
import jax.numpy as jnp
from jax import lax
from jax.experimental import pallas as pl
from jax.experimental.pallas import tpu as pltpu
from jax.sharding import PartitionSpec as P


HEADS = 32
KV_HEADS = 8
HEAD_DIM = 128
GROUP = HEADS // KV_HEADS
FACTOR = HEAD_DIM ** (-0.5)
F32 = jnp.float32
BF16 = jnp.bfloat16


def dot_nt(a, b):
    return lax.dot_general(a, b, (((1,), (1,)), ((), ())), preferred_element_type=F32)


def make_plain():
    def local(activations, grad_out, query_weight, key_weight, value_weight):
        gathered = tuple(
            lax.all_gather(w, "seq", axis=0, tiled=True)
            for w in (query_weight, key_weight, value_weight)
        )
        tokens = activations.shape[0]
        whole = lax.all_gather(activations, "head", axis=1, tiled=True)
        queries, keys, values = (
            jnp.dot(whole, w, preferred_element_type=F32).astype(BF16) for w in gathered
        )
        groups = keys.shape[1] // HEAD_DIM
        q = queries.reshape(tokens, groups, GROUP, HEAD_DIM)
        k = keys.reshape(tokens, groups, HEAD_DIM)
        v = values.reshape(tokens, groups, HEAD_DIM)
        do = grad_out.reshape(tokens, groups, GROUP, HEAD_DIM)
        kv_state = jnp.einsum("tgd,tge->gde", k, v, preferred_element_type=F32).astype(BF16)
        grad_state = (
            FACTOR * jnp.einsum("tghd,tghe->gde", q, do, preferred_element_type=F32)
        ).astype(BF16)
        every_kv = lax.all_gather(kv_state[None], "seq", axis=0, tiled=True)
        every_grad = lax.all_gather(grad_state[None], "seq", axis=0, tiled=True)
        position = lax.axis_index("seq")
        order = jnp.arange(every_kv.shape[0], dtype=jnp.int32)
        before = (order < position).astype(BF16)
        after = (order > position).astype(BF16)
        prefix = jnp.einsum("n,ngde->gde", before, every_kv, preferred_element_type=F32).astype(BF16)
        suffix = jnp.einsum("n,ngde->gde", after, every_grad, preferred_element_type=F32).astype(BF16)
        causal = jnp.arange(tokens)[:, None] >= jnp.arange(tokens)[None, :]
        s = jnp.where(
            causal, jnp.einsum("tghd,sgd->ghts", q, k, preferred_element_type=F32), 0.0
        ).astype(BF16)
        ds = jnp.where(
            causal, jnp.einsum("tghe,sge->ghts", do, v, preferred_element_type=F32), 0.0
        ).astype(BF16)
        grad_query = FACTOR * (
            jnp.einsum("ghts,sgd->tghd", ds, k, preferred_element_type=F32)
            + jnp.einsum("tghe,gde->tghd", do, prefix, preferred_element_type=F32)
        )
        grad_key = FACTOR * jnp.einsum(
            "ghts,tghd->sgd", ds, q, preferred_element_type=F32
        ) + jnp.einsum("sge,gde->sgd", v, suffix, preferred_element_type=F32)
        grad_value = FACTOR * jnp.einsum(
            "ghts,tghe->sge", s, do, preferred_element_type=F32
        ) + jnp.einsum("sgd,gde->sge", k, suffix, preferred_element_type=F32)
        parts = (
            dot_nt(g.astype(BF16).reshape(tokens, -1), w)
            for g, w in zip((grad_query, grad_key, grad_value), gathered)
        )
        return lax.psum_scatter(
            sum(parts).astype(BF16), "head", scatter_dimension=1, tiled=True
        )

    return local


def mm(a, b, contract):
    return lax.dot_general(a, b, (contract, ((), ())), preferred_element_type=F32)


NN, NT, TN = ((1,), (0,)), ((1,), (1,)), ((0,), (0,))


def head_cols(h):
    return slice(h * HEAD_DIM, (h + 1) * HEAD_DIM)


def state_kernel(kv_ref, out_ref, total_ref):
    tokens = kv_ref.shape[0] // 2
    for g in range(out_ref.shape[1]):
        total = jnp.zeros(total_ref.shape[1:], F32)
        for n in range(out_ref.shape[0]):
            t = slice(n * tokens, (n + 1) * tokens)
            k, v = kv_ref[t, head_cols(2 * g)], kv_ref[t, head_cols(2 * g + 1)]
            state = mm(k, v, TN).astype(BF16)
            out_ref[n, g] = state
            total = total + state.astype(F32)
        total_ref[g] = total.astype(BF16)


def scores_mask(n):
    return lax.broadcasted_iota(jnp.int32, (n, n), 0) <= lax.broadcasted_iota(
        jnp.int32, (n, n), 1
    )


def grad_query_kernel(k_ref, v_ref, do_ref, prefix_ref, out_ref):
    k, v, prefix = k_ref[...], v_ref[...], prefix_ref[0, 0]
    shape = (k.shape[0], k.shape[0])
    mask = lax.broadcasted_iota(jnp.int32, shape, 0) >= lax.broadcasted_iota(jnp.int32, shape, 1)
    for h in range(GROUP):
        do = do_ref[:, head_cols(h)]
        ds = jnp.where(mask, mm(do, v, NT), 0.0).astype(BF16)
        out_ref[:, head_cols(h)] = (FACTOR * (mm(ds, k, NN) + mm(do, prefix, NT))).astype(BF16)


def inner_kernel(q_ref, k_ref, v_ref, do_ref, out_ref):
    k, v = k_ref[...], v_ref[...]
    mask = scores_mask(k.shape[0])
    gk = jnp.zeros(k.shape, F32)
    gv = jnp.zeros(k.shape, F32)
    for h in range(GROUP):
        q, do = q_ref[:, head_cols(h)], do_ref[:, head_cols(h)]
        ds = jnp.where(mask, mm(v, do, NT), 0.0).astype(BF16)
        s = jnp.where(mask, mm(k, q, NT), 0.0).astype(BF16)
        gk = gk + mm(ds, q, NN)
        gv = gv + mm(s, do, NN)
    out_ref[:, head_cols(0)] = FACTOR * gk
    out_ref[:, head_cols(1)] = FACTOR * gv


def outer_kernel(flag_ref, kv_ref, outside_ref, got_ref, state_ref, *refs):
    inner_refs, out_refs = refs[:-2], refs[-2:]
    tokens = kv_ref.shape[0] // 2
    for g, inner_ref in enumerate(inner_refs):
        behind = outside_ref[g] + jnp.where(flag_ref[0] == 1, got_ref[g].astype(F32), 0.0)
        for n in range(2):
            add = (flag_ref[1] == 1) if n == 0 else (flag_ref[1] == 0)
            suffix = behind + jnp.where(add, state_ref[1 - n, g].astype(F32), 0.0)
            suffix = suffix.astype(BF16)
            t = slice(n * tokens, (n + 1) * tokens)
            k, v = kv_ref[t, head_cols(2 * g)], kv_ref[t, head_cols(2 * g + 1)]
            gk = inner_ref[t, head_cols(0)] + mm(v, suffix, NT)
            gv = inner_ref[t, head_cols(1)] + mm(k, suffix, NN)
            out_refs[n][:, head_cols(2 * g)] = gk.astype(BF16)
            out_refs[n][:, head_cols(2 * g + 1)] = gv.astype(BF16)


def project_call(base, x, weights, total, dtype, do=None):
    slots = sorted(weights)
    pieces = [weights[i] if isinstance(weights[i], tuple) else (weights[i],) for i in slots]
    cols = pieces[0][0].shape[1]
    rows = sum(w.shape[0] for w in pieces[0])
    tokens = x.shape[0] // 2
    width = GROUP * HEAD_DIM if do is not None else rows // 2
    n = len(slots)

    def body(base_ref, *refs):
        xs, rest = refs[:n], list(refs[n:])
        ws = [[rest.pop(0) for _ in piece] for piece in pieces]
        acc = rest.pop(0)[...] if total is not None else None
        do_ref = rest.pop(0) if do is not None else None
        for x_ref, w_refs in zip(xs, ws):
            at = 0
            for w_ref in w_refs:
                part = mm(x_ref[:, at : at + w_ref.shape[0]], w_ref[...], NN)
                acc = part if acc is None else acc + part
                at += w_ref.shape[0]
        acc = acc.astype(dtype)
        rest[0][...] = acc
        if do_ref is not None:
            both = None
            for m in range(2):
                t = slice(m * tokens, (m + 1) * tokens)
                state = None
                for h in range(GROUP):
                    part = mm(acc[t, head_cols(h)], do_ref[t, head_cols(h)], TN)
                    state = part if state is None else state + part
                state = (FACTOR * state).astype(BF16)
                rest[1][m, 0] = state
                state = state.astype(F32)
                both = state if both is None else both + state
            rest[2][0] = both.astype(BF16)

    def x_spec(i):
        return pl.BlockSpec((2 * tokens, rows), lambda j, b: (0, b[0] ^ i))

    tile = pl.BlockSpec((2 * tokens, width), lambda j, b: (0, j))
    args = [x] * n + [w for piece in pieces for w in piece]
    in_specs = [x_spec(i) for i in slots]
    in_specs += [
        pl.BlockSpec((w.shape[0], width), lambda j, b: (0, j)) for piece in pieces for w in piece
    ]
    out_shape, out_specs = [jax.ShapeDtypeStruct((2 * tokens, cols), dtype)], [tile]
    if total is not None:
        args.append(total)
        in_specs.append(tile)
    if do is not None:
        args.append(do)
        in_specs.append(tile)
        one = (cols // width, HEAD_DIM, HEAD_DIM)
        out_shape += [jax.ShapeDtypeStruct((2,) + one, BF16), jax.ShapeDtypeStruct(one, BF16)]
        out_specs += [
            pl.BlockSpec((2, 1, HEAD_DIM, HEAD_DIM), lambda j, b: (0, j, 0, 0)),
            pl.BlockSpec((1, HEAD_DIM, HEAD_DIM), lambda j, b: (j, 0, 0)),
        ]
    out = pl.pallas_call(
        body,
        out_shape=out_shape,
        grid_spec=pltpu.PrefetchScalarGridSpec(
            num_scalar_prefetch=1,
            grid=(cols // width,),
            in_specs=in_specs,
            out_specs=out_specs,
        ),
    )(base, *args)
    return out if do is not None else out[0]


def back_call(side, grads, low, high):
    n = len(low)
    pieces = [w if isinstance(w, tuple) else (w,) for w in low + high]
    rows = sum(w.shape[0] for w in pieces[0])
    inner = grads.shape[1]
    tokens = grads.shape[0] // 2
    half = rows // 2

    def body(side_ref, g_ref, *refs):
        rest, (keep_ref, send_ref) = list(refs[:-2]), refs[-2:]
        first = pl.program_id(0) == 0
        for m, piece in enumerate(pieces):
            w = [rest.pop(0)[...] for _ in piece]
            if len(w) > 1:
                w = jnp.concatenate(w, 0)
                w = jnp.where(first, w[:half], w[half:])
            else:
                w = w[0]
            both = mm(g_ref[...], w, NT)
            where = side_ref[0] if m < n else 1 - side_ref[0]
            keep_ref[where, m % n] = both[:tokens]
            send_ref[where, m % n] = both[tokens:].astype(BF16)

    in_specs = [pl.BlockSpec(grads.shape, lambda j, b: (0, 0))]
    for piece in pieces:
        if len(piece) == 1:
            in_specs.append(pl.BlockSpec((half, inner), lambda j, b: (j, 0)))
        else:
            in_specs += [pl.BlockSpec(w.shape, lambda j, b: (0, 0)) for w in piece]
    out = pl.BlockSpec((2, n, tokens, half), lambda j, b: (0, 0, 0, j))
    shape = (2, n, tokens, rows)
    return pl.pallas_call(
        body,
        out_shape=(jax.ShapeDtypeStruct(shape, F32), jax.ShapeDtypeStruct(shape, BF16)),
        grid_spec=pltpu.PrefetchScalarGridSpec(
            num_scalar_prefetch=1, grid=(2,), in_specs=in_specs, out_specs=(out, out)
        ),
    )(side, grads, *(w for piece in pieces for w in piece))


def add_two(total, g, g_other, w, w_other):
    return total + mm(g, w, NT) + mm(g_other, w_other, NT)


def home_kernel(sum_ref, g_ref, g_other_ref, w_ref, w_other_ref, out_ref):
    out_ref[0] = add_two(
        sum_ref[0], g_ref[...], g_other_ref[...], w_ref[...], w_other_ref[...]
    )


def finish_kernel(base_ref, sum_ref, g_ref, g_other_ref, w_ref, w_other_ref, out_ref):
    slots, _, width = sum_ref.shape
    for i in range(slots):
        at = base_ref[0] ^ i
        out_ref[:, i * width : (i + 1) * width] = add_two(
            sum_ref[at], g_ref[...], g_other_ref[...], w_ref[at], w_other_ref[at]
        ).astype(BF16)


def make_split(zs, xs, ys):
    n_seq = zs * xs * 2

    def swap(value, bit):
        return lax.ppermute(value, "seq", [(s, s ^ bit) for s in range(n_seq)])

    def swap_y(value):
        return lax.ppermute(value, "head", [(y, y ^ 1) for y in range(ys)])

    Z1, Z2, X1, C1 = 2 * xs, 4 * xs, 2, 1

    def local(activations, grad_out, query_weight, key_weight, value_weight):
        tokens, _ = activations.shape
        groups = key_weight.shape[1] // HEAD_DIM // 2
        seq = lax.axis_index("seq")
        y = lax.axis_index("head")
        core, x, z = seq % 2, (seq // 2) % xs, seq // (2 * xs)
        chip, chips = seq // 2, n_seq // 2
        per_half = chips // ys
        side = (chip // per_half) ^ y

        def cols(w, which):
            n = w.shape[1] // 2
            return lax.dynamic_slice_in_dim(w, which * n, n, 1)

        def own_and_other(own, other):
            return jnp.concatenate([own, swap(other, C1)], 0)

        def in_order(own, other):
            n = own.shape[0]
            both = jnp.zeros((2 * n, own.shape[1]), own.dtype)
            both = lax.dynamic_update_slice_in_dim(both, own, core * n, 0)
            got = swap(other, C1)
            return lax.dynamic_update_slice_in_dim(both, got, (1 - core) * n, 0)

        def keys_and_values(which):
            k, v = cols(key_weight, which), cols(value_weight, which)
            return jnp.concatenate(
                [w[:, head_cols(g)] for g in range(groups) for w in (k, v)], 1
            )

        def gate(value, *first):
            return lax.optimization_barrier((value,) + first)[0]

        def scalar(value):
            return value.reshape(1).astype(jnp.int32)

        chunk_a = in_order(keys_and_values(core), keys_and_values(1 - core))
        chunk_b = in_order(cols(query_weight, core), cols(query_weight, 1 - core))
        do_all = own_and_other(cols(grad_out, core), cols(grad_out, 1 - core))
        acts = jnp.concatenate([activations, swap_y(activations)], 1)
        acts = gate(own_and_other(acts, acts), do_all)
        base = scalar(side * per_half + chip % per_half)

        def project(weights, which, total, dtype, do=None):
            return project_call(
                base, acts, {i: weights[i] for i in which}, total, dtype, do
            )

        w_kv, w_q = [chunk_a] + [None] * (chips - 1), [chunk_b] + [None] * (chips - 1)
        w_kv[4], w_kv[2] = swap(chunk_a, Z2), swap(chunk_a, Z1)
        w_kv[1] = swap(chunk_a, X1)
        w_q[1] = (swap(chunk_b[:tokens], X1), swap(chunk_b[tokens:], X1))
        w_kv[6] = swap(w_kv[4], Z1)
        w_q[4], w_q[2] = swap(chunk_b, Z2), swap(chunk_b, Z1)
        w_kv[3], w_kv[5] = swap(w_kv[2], X1), swap(w_kv[4], X1)
        w_kv[7] = swap(w_kv[6], X1)
        kv_sum = project(w_kv, (0, 1, 2, 4), None, F32)
        w_q[5], w_q[6] = swap(w_q[4], X1), swap(w_q[4], Z1)
        kv = project(w_kv, (3, 5, 6, 7), kv_sum, BF16)
        w_q[3] = swap(w_q[2], X1)
        q_sum = project(w_q, (0, 1, 2, 4), None, F32)
        cut = tokens // 2
        w_q[7] = (swap(w_q[6][:cut], X1), swap(w_q[5][cut:], Z1))

        n_half = chips // ys
        low, high = jnp.concatenate(w_kv[:n_half], 0), jnp.concatenate(w_kv[n_half:], 0)
        w_home = jnp.where(side == 0, low, high)
        w_home_y = swap_y(jnp.where(side == 0, high, low))
        w_home_c = swap(w_home, C1)
        w_home_cy = swap(w_home_y, C1)

        n_cols = GROUP * HEAD_DIM
        states = jax.ShapeDtypeStruct((2, groups, HEAD_DIM, HEAD_DIM), BF16)

        def scan(total, ahead):
            total = total.astype(F32)
            outside = jnp.zeros_like(total)
            for bit, at in ((X1, x), (Z1, z % 2), (Z2, z // 2)):
                got = swap(total.astype(BF16), bit)
                counts = (at == 1) == ahead
                if bit == Z2:
                    return outside, got, counts
                outside = outside + jnp.where(counts, got.astype(F32), 0.0)
                total = total + got.astype(F32)

        totals = jax.ShapeDtypeStruct(states.shape[1:], BF16)
        state, total = pl.pallas_call(state_kernel, out_shape=(states, totals))(kv)
        outside, got, counts = scan(total, True)
        outside = outside + jnp.where(counts, got.astype(F32), 0.0)
        prefix = jnp.stack(
            [
                outside + jnp.where(core == 1, state[1].astype(F32), 0.0),
                outside + jnp.where(core == 0, state[0].astype(F32), 0.0),
            ]
        ).astype(BF16)
        q_spec = pl.BlockSpec((tokens, n_cols), lambda n, g: (n, g))
        gq = pl.pallas_call(
            grad_query_kernel,
            out_shape=jax.ShapeDtypeStruct((2 * tokens, groups * n_cols), BF16),
            grid=(2, groups),
            in_specs=[
                pl.BlockSpec((tokens, HEAD_DIM), lambda n, g: (n, 2 * g)),
                pl.BlockSpec((tokens, HEAD_DIM), lambda n, g: (n, 2 * g + 1)),
                q_spec,
                pl.BlockSpec((1, 1, HEAD_DIM, HEAD_DIM), lambda n, g: (n, g, 0, 0)),
            ],
            out_specs=q_spec,
        )(kv, kv, do_all, prefix)

        def back(which, after=None):
            keep, send = back_call(
                scalar(side), gq, [w_q[i] for i in which], [w_q[i + n_half] for i in which]
            )
            got = swap(send, C1)
            if after is not None:
                keep = gate(keep, after)
            away = (keep[1] + got[1].astype(F32)).astype(BF16)
            return keep[0], got[0], swap_y(away), away

        sums = [back((0, 1))]
        sums.append(back((2,), sums[0][3]))
        q_sum = project(w_q, (5, 6), q_sum, F32)
        q, gs, total = project(w_q, (3, 7), q_sum, BF16, do_all)
        outside, got, counts = scan(total, False)
        inner = []
        for g in range(groups):
            inner.append(
                pl.pallas_call(
                    inner_kernel,
                    out_shape=jax.ShapeDtypeStruct((2 * tokens, 2 * HEAD_DIM), F32),
                    grid=(2,),
                    in_specs=[
                        pl.BlockSpec((tokens, n_cols), lambda n, g=g: (n, g)),
                        pl.BlockSpec((tokens, HEAD_DIM), lambda n, g=g: (n, 2 * g)),
                        pl.BlockSpec((tokens, HEAD_DIM), lambda n, g=g: (n, 2 * g + 1)),
                        pl.BlockSpec((tokens, n_cols), lambda n, g=g: (n, g)),
                    ],
                    out_specs=pl.BlockSpec((tokens, 2 * HEAD_DIM), lambda n: (n, 0)),
                )(q, kv, kv, do_all)
            )
        sums.append(back((3,)))
        flags = jnp.stack([counts, core == 0]).astype(jnp.int32)
        part = jax.ShapeDtypeStruct((tokens, 2 * groups * HEAD_DIM), BF16)
        vmem = pl.BlockSpec(memory_space=pltpu.VMEM)
        gkv, gkv_other = pl.pallas_call(
            outer_kernel,
            out_shape=(part, part),
            in_specs=[pl.BlockSpec(memory_space=pltpu.SMEM)] + [vmem] * (4 + groups),
            out_specs=(vmem, vmem),
        )(flags, kv, outside, got, gs, *inner)
        far_other, far = swap_y(gkv_other), swap_y(gkv)
        gkv_c, far_c = swap(gkv_other, C1), swap(far_other, C1)
        home = jnp.concatenate(
            [p[0] + p[1].astype(F32) + p[2].astype(F32) for p in sums], 0
        )
        slots, width = home.shape[0], home.shape[2]
        home = pl.pallas_call(
            home_kernel,
            out_shape=jax.ShapeDtypeStruct(home.shape, F32),
            grid=(slots,),
            in_specs=[pl.BlockSpec((1, tokens, width), lambda i: (i, 0, 0))]
            + [pl.BlockSpec(gkv.shape, lambda i: (0, 0))] * 2
            + [pl.BlockSpec((width, w_home.shape[1]), lambda i: (i, 0))] * 2,
            out_specs=pl.BlockSpec((1, tokens, width), lambda i: (i, 0, 0)),
        )(home, gkv, gkv_c, w_home, w_home_c)
        by_slot = (slots, width, w_home.shape[1])
        return pl.pallas_call(
            finish_kernel,
            out_shape=jax.ShapeDtypeStruct((tokens, slots * width), BF16),
            in_specs=[pl.BlockSpec(memory_space=pltpu.SMEM)] + [vmem] * 5,
            out_specs=vmem,
        )(
            scalar(chip % per_half),
            home,
            far,
            far_c,
            w_home_y.reshape(by_slot),
            w_home_cy.reshape(by_slot),
        )

    return local


def solution(mesh):
    n_seq, n_head = mesh.shape["seq"], mesh.shape["head"]
    groups = KV_HEADS // n_head
    split = n_seq == 4 * 2 * 2 and groups % 2 == 0 and n_head == 2
    local = make_split(n_seq // 4, 2, n_head) if split else make_plain()

    spec = P("seq", "head")
    return jax.shard_map(local, mesh=mesh, in_specs=(spec,) * 5, out_specs=spec, check_vma=False)
```

```python
import jax
import jax.numpy as jnp
from jax import lax
from jax.experimental import pallas as pl
from jax.experimental.pallas import tpu as pltpu
from jax.sharding import PartitionSpec as P


HEADS = 32
KV_HEADS = 8
HEAD_DIM = 128
GROUP = HEADS // KV_HEADS
FACTOR = HEAD_DIM ** (-0.5)
F32 = jnp.float32
BF16 = jnp.bfloat16


def kernel_call(body, **kwargs):
    return pl.pallas_call(
        body, compiler_params=pltpu.CompilerParams(vmem_limit_bytes=20 * 2**20), **kwargs
    )


def dot_nt(a, b):
    return lax.dot_general(a, b, (((1,), (1,)), ((), ())), preferred_element_type=F32)


def make_plain():
    def local(activations, grad_out, query_weight, key_weight, value_weight):
        gathered = tuple(
            lax.all_gather(w, "seq", axis=0, tiled=True)
            for w in (query_weight, key_weight, value_weight)
        )
        tokens = activations.shape[0]
        whole = lax.all_gather(activations, "head", axis=1, tiled=True)
        queries, keys, values = (
            jnp.dot(whole, w, preferred_element_type=F32).astype(BF16) for w in gathered
        )
        groups = keys.shape[1] // HEAD_DIM
        q = queries.reshape(tokens, groups, GROUP, HEAD_DIM)
        k = keys.reshape(tokens, groups, HEAD_DIM)
        v = values.reshape(tokens, groups, HEAD_DIM)
        do = grad_out.reshape(tokens, groups, GROUP, HEAD_DIM)
        kv_state = jnp.einsum("tgd,tge->gde", k, v, preferred_element_type=F32).astype(BF16)
        grad_state = (
            FACTOR * jnp.einsum("tghd,tghe->gde", q, do, preferred_element_type=F32)
        ).astype(BF16)
        every_kv = lax.all_gather(kv_state[None], "seq", axis=0, tiled=True)
        every_grad = lax.all_gather(grad_state[None], "seq", axis=0, tiled=True)
        position = lax.axis_index("seq")
        order = jnp.arange(every_kv.shape[0], dtype=jnp.int32)
        before = (order < position).astype(BF16)
        after = (order > position).astype(BF16)
        prefix = jnp.einsum("n,ngde->gde", before, every_kv, preferred_element_type=F32).astype(BF16)
        suffix = jnp.einsum("n,ngde->gde", after, every_grad, preferred_element_type=F32).astype(BF16)
        causal = jnp.arange(tokens)[:, None] >= jnp.arange(tokens)[None, :]
        s = jnp.where(
            causal, jnp.einsum("tghd,sgd->ghts", q, k, preferred_element_type=F32), 0.0
        ).astype(BF16)
        ds = jnp.where(
            causal, jnp.einsum("tghe,sge->ghts", do, v, preferred_element_type=F32), 0.0
        ).astype(BF16)
        grad_query = FACTOR * (
            jnp.einsum("ghts,sgd->tghd", ds, k, preferred_element_type=F32)
            + jnp.einsum("tghe,gde->tghd", do, prefix, preferred_element_type=F32)
        )
        grad_key = FACTOR * jnp.einsum(
            "ghts,tghd->sgd", ds, q, preferred_element_type=F32
        ) + jnp.einsum("sge,gde->sgd", v, suffix, preferred_element_type=F32)
        grad_value = FACTOR * jnp.einsum(
            "ghts,tghe->sge", s, do, preferred_element_type=F32
        ) + jnp.einsum("sgd,gde->sge", k, suffix, preferred_element_type=F32)
        parts = (
            dot_nt(g.astype(BF16).reshape(tokens, -1), w)
            for g, w in zip((grad_query, grad_key, grad_value), gathered)
        )
        return lax.psum_scatter(
            sum(parts).astype(BF16), "head", scatter_dimension=1, tiled=True
        )

    return local


def mm(a, b, contract):
    return lax.dot_general(a, b, (contract, ((), ())), preferred_element_type=F32)


NN, NT, TN = ((1,), (0,)), ((1,), (1,)), ((0,), (0,))


def head_cols(h):
    return slice(h * HEAD_DIM, (h + 1) * HEAD_DIM)


def state_kernel(kv_ref, out_ref, total_ref):
    tokens = kv_ref.shape[0] // 2
    for g in range(out_ref.shape[1]):
        total = jnp.zeros(total_ref.shape[1:], F32)
        for n in range(out_ref.shape[0]):
            t = slice(n * tokens, (n + 1) * tokens)
            k, v = kv_ref[t, head_cols(2 * g)], kv_ref[t, head_cols(2 * g + 1)]
            state = mm(k, v, TN).astype(BF16)
            out_ref[n, g] = state
            total = total + state.astype(F32)
        total_ref[g] = total.astype(BF16)


def scores_mask(n):
    return lax.broadcasted_iota(jnp.int32, (n, n), 0) <= lax.broadcasted_iota(
        jnp.int32, (n, n), 1
    )


def grad_query_kernel(k_ref, v_ref, do_ref, prefix_ref, out_ref):
    k, v, prefix = k_ref[...], v_ref[...], prefix_ref[0, 0]
    shape = (k.shape[0], k.shape[0])
    mask = lax.broadcasted_iota(jnp.int32, shape, 0) >= lax.broadcasted_iota(jnp.int32, shape, 1)
    for h in range(GROUP):
        do = do_ref[:, head_cols(h)]
        ds = jnp.where(mask, mm(do, v, NT), 0.0).astype(BF16)
        out_ref[:, head_cols(h)] = (FACTOR * (mm(ds, k, NN) + mm(do, prefix, NT))).astype(BF16)


def inner_kernel(q_ref, k_ref, v_ref, do_ref, out_ref):
    k, v = k_ref[...], v_ref[...]
    mask = scores_mask(k.shape[0])
    gk = jnp.zeros(k.shape, F32)
    gv = jnp.zeros(k.shape, F32)
    for h in range(GROUP):
        q, do = q_ref[:, head_cols(h)], do_ref[:, head_cols(h)]
        ds = jnp.where(mask, mm(v, do, NT), 0.0).astype(BF16)
        s = jnp.where(mask, mm(k, q, NT), 0.0).astype(BF16)
        gk = gk + mm(ds, q, NN)
        gv = gv + mm(s, do, NN)
    out_ref[:, head_cols(0)] = FACTOR * gk
    out_ref[:, head_cols(1)] = FACTOR * gv


def outer_kernel(flag_ref, kv_ref, outside_ref, got_ref, state_ref, *refs):
    inner_refs, out_refs = refs[:-2], refs[-2:]
    tokens = kv_ref.shape[0] // 2
    for g, inner_ref in enumerate(inner_refs):
        behind = outside_ref[g] + jnp.where(flag_ref[0] == 1, got_ref[g].astype(F32), 0.0)
        for n in range(2):
            add = (flag_ref[1] == 1) if n == 0 else (flag_ref[1] == 0)
            suffix = behind + jnp.where(add, state_ref[1 - n, g].astype(F32), 0.0)
            suffix = suffix.astype(BF16)
            t = slice(n * tokens, (n + 1) * tokens)
            k, v = kv_ref[t, head_cols(2 * g)], kv_ref[t, head_cols(2 * g + 1)]
            gk = inner_ref[t, head_cols(0)] + mm(v, suffix, NT)
            gv = inner_ref[t, head_cols(1)] + mm(k, suffix, NN)
            out_refs[n][:, head_cols(2 * g)] = gk.astype(BF16)
            out_refs[n][:, head_cols(2 * g + 1)] = gv.astype(BF16)


def project_call(base, x, weights, total, dtype, do=None):
    slots = sorted(weights)
    pieces = [weights[i] if isinstance(weights[i], tuple) else (weights[i],) for i in slots]
    cols = pieces[0][0].shape[1]
    rows = sum(w.shape[0] for w in pieces[0])
    tokens = x.shape[0] // 2
    width = GROUP * HEAD_DIM if do is not None else rows // 2
    n = len(slots)

    def body(base_ref, *refs):
        xs, rest = refs[:n], list(refs[n:])
        ws = [[rest.pop(0) for _ in piece] for piece in pieces]
        acc = rest.pop(0)[...] if total is not None else None
        do_ref = rest.pop(0) if do is not None else None
        for x_ref, w_refs in zip(xs, ws):
            at = 0
            for w_ref in w_refs:
                part = mm(x_ref[:, at : at + w_ref.shape[0]], w_ref[...], NN)
                acc = part if acc is None else acc + part
                at += w_ref.shape[0]
        acc = acc.astype(dtype)
        rest[0][...] = acc
        if do_ref is not None:
            both = None
            for m in range(2):
                t = slice(m * tokens, (m + 1) * tokens)
                state = None
                for h in range(GROUP):
                    part = mm(acc[t, head_cols(h)], do_ref[t, head_cols(h)], TN)
                    state = part if state is None else state + part
                state = (FACTOR * state).astype(BF16)
                rest[1][m, 0] = state
                state = state.astype(F32)
                both = state if both is None else both + state
            rest[2][0] = both.astype(BF16)

    def x_spec(i):
        return pl.BlockSpec((2 * tokens, rows), lambda j, b: (0, b[0] ^ i))

    tile = pl.BlockSpec((2 * tokens, width), lambda j, b: (0, j))
    args = [x] * n + [w for piece in pieces for w in piece]
    in_specs = [x_spec(i) for i in slots]
    in_specs += [
        pl.BlockSpec((w.shape[0], width), lambda j, b: (0, j)) for piece in pieces for w in piece
    ]
    out_shape, out_specs = [jax.ShapeDtypeStruct((2 * tokens, cols), dtype)], [tile]
    if total is not None:
        args.append(total)
        in_specs.append(tile)
    if do is not None:
        args.append(do)
        in_specs.append(tile)
        one = (cols // width, HEAD_DIM, HEAD_DIM)
        out_shape += [jax.ShapeDtypeStruct((2,) + one, BF16), jax.ShapeDtypeStruct(one, BF16)]
        out_specs += [
            pl.BlockSpec((2, 1, HEAD_DIM, HEAD_DIM), lambda j, b: (0, j, 0, 0)),
            pl.BlockSpec((1, HEAD_DIM, HEAD_DIM), lambda j, b: (j, 0, 0)),
        ]
    out = kernel_call(
        body,
        out_shape=out_shape,
        grid_spec=pltpu.PrefetchScalarGridSpec(
            num_scalar_prefetch=1,
            grid=(cols // width,),
            in_specs=in_specs,
            out_specs=out_specs,
        ),
    )(base, *args)
    return out if do is not None else out[0]


def back_call(side, grads, low, high):
    n = len(low)
    pieces = [w if isinstance(w, tuple) else (w,) for w in low + high]
    rows = sum(w.shape[0] for w in pieces[0])
    inner = grads.shape[1]
    tokens = grads.shape[0] // 2
    half = rows // 2

    def body(side_ref, g_ref, *refs):
        rest, (keep_ref, send_ref) = list(refs[:-2]), refs[-2:]
        first = pl.program_id(0) == 0
        for m, piece in enumerate(pieces):
            w = [rest.pop(0)[...] for _ in piece]
            if len(w) > 1:
                w = jnp.concatenate(w, 0)
                w = jnp.where(first, w[:half], w[half:])
            else:
                w = w[0]
            both = mm(g_ref[...], w, NT)
            where = side_ref[0] if m < n else 1 - side_ref[0]
            keep_ref[where, m % n] = both[:tokens]
            send_ref[where, m % n] = both[tokens:].astype(BF16)

    in_specs = [pl.BlockSpec(grads.shape, lambda j, b: (0, 0))]
    for piece in pieces:
        if len(piece) == 1:
            in_specs.append(pl.BlockSpec((half, inner), lambda j, b: (j, 0)))
        else:
            in_specs += [pl.BlockSpec(w.shape, lambda j, b: (0, 0)) for w in piece]
    out = pl.BlockSpec((2, n, tokens, half), lambda j, b: (0, 0, 0, j))
    shape = (2, n, tokens, rows)
    return kernel_call(
        body,
        out_shape=(jax.ShapeDtypeStruct(shape, F32), jax.ShapeDtypeStruct(shape, BF16)),
        grid_spec=pltpu.PrefetchScalarGridSpec(
            num_scalar_prefetch=1, grid=(2,), in_specs=in_specs, out_specs=(out, out)
        ),
    )(side, grads, *(w for piece in pieces for w in piece))


def add_two(total, g, g_other, w, w_other):
    return total + mm(g, w, NT) + mm(g_other, w_other, NT)


def home_kernel(g_ref, g_other_ref, w_ref, w_other_ref, *refs):
    out_ref, triples = refs[-1], [refs[i : i + 3] for i in range(0, len(refs) - 1, 3)]
    slot = pl.program_id(0)
    total = None
    for n, (keep, core, far) in enumerate(triples):
        part = keep[0, 0] + core[0, 0].astype(F32) + far[0].astype(F32)
        total = part if total is None else jnp.where(slot > n, part, total)
    out_ref[0] = add_two(total, g_ref[...], g_other_ref[...], w_ref[...], w_other_ref[...])


def fetch_kernel(*refs):
    n = (len(refs) - 1) // 2
    sems = refs[-1]
    copies = [pltpu.make_async_copy(refs[i], refs[n + i], sems.at[i]) for i in range(n)]
    for copy in copies:
        copy.start()
    for copy in copies:
        copy.wait()


def fetch(*arrays):
    hbm = pl.BlockSpec(memory_space=pl.ANY)
    vmem = pl.BlockSpec(memory_space=pltpu.VMEM)
    return kernel_call(
        fetch_kernel,
        out_shape=[pltpu.VMEM(a.shape, a.dtype) for a in arrays],
        in_specs=[hbm] * len(arrays),
        out_specs=[vmem] * len(arrays),
        scratch_shapes=[pltpu.SemaphoreType.DMA((len(arrays),))],
    )(*arrays)


def finish_kernel(base_ref, sum_ref, g_ref, g_other_ref, w_ref, w_other_ref, out_ref):
    slots, _, width = sum_ref.shape
    for i in range(slots):
        at = base_ref[0] ^ i
        out_ref[:, i * width : (i + 1) * width] = add_two(
            sum_ref[at], g_ref[...], g_other_ref[...], w_ref[at], w_other_ref[at]
        ).astype(BF16)


def make_split(zs, xs, ys):
    n_seq = zs * xs * 2

    def swap(value, bit):
        return lax.ppermute(value, "seq", [(s, s ^ bit) for s in range(n_seq)])

    def swap_y(value):
        return lax.ppermute(value, "head", [(y, y ^ 1) for y in range(ys)])

    Z1, Z2, X1, C1 = 2 * xs, 4 * xs, 2, 1

    def local(activations, grad_out, query_weight, key_weight, value_weight):
        tokens, _ = activations.shape
        groups = key_weight.shape[1] // HEAD_DIM // 2
        seq = lax.axis_index("seq")
        y = lax.axis_index("head")
        core, x, z = seq % 2, (seq // 2) % xs, seq // (2 * xs)
        chip, chips = seq // 2, n_seq // 2
        per_half = chips // ys
        side = (chip // per_half) ^ y

        def cols(w, which):
            n = w.shape[1] // 2
            return lax.dynamic_slice_in_dim(w, which * n, n, 1)

        def own_and_other(own, other):
            return jnp.concatenate([own, swap(other, C1)], 0)

        def in_order(own, other):
            n = own.shape[0]
            both = jnp.zeros((2 * n, own.shape[1]), own.dtype)
            both = lax.dynamic_update_slice_in_dim(both, own, core * n, 0)
            got = swap(other, C1)
            return lax.dynamic_update_slice_in_dim(both, got, (1 - core) * n, 0)

        def keys_and_values(which):
            k, v = cols(key_weight, which), cols(value_weight, which)
            return jnp.concatenate(
                [w[:, head_cols(g)] for g in range(groups) for w in (k, v)], 1
            )

        def gate(value, *first):
            return lax.optimization_barrier((value,) + first)[0]

        def scalar(value):
            return value.reshape(1).astype(jnp.int32)

        chunk_a = in_order(keys_and_values(core), keys_and_values(1 - core))
        chunk_b = in_order(cols(query_weight, core), cols(query_weight, 1 - core))
        do_all = own_and_other(cols(grad_out, core), cols(grad_out, 1 - core))
        acts = jnp.concatenate([activations, swap_y(activations)], 1)
        acts = gate(own_and_other(acts, acts), do_all)
        base = scalar(side * per_half + chip % per_half)

        def project(weights, which, total, dtype, do=None):
            return project_call(
                base, acts, {i: weights[i] for i in which}, total, dtype, do
            )

        w_kv, w_q = [chunk_a] + [None] * (chips - 1), [chunk_b] + [None] * (chips - 1)
        w_kv[4], w_kv[2] = swap(chunk_a, Z2), swap(chunk_a, Z1)
        w_kv[1] = swap(chunk_a, X1)
        w_q[1] = (swap(chunk_b[:tokens], X1), swap(chunk_b[tokens:], X1))
        w_kv[6] = swap(w_kv[4], Z1)
        w_q[4], w_q[2] = swap(chunk_b, Z2), swap(chunk_b, Z1)
        w_kv[3], w_kv[5] = swap(w_kv[2], X1), swap(w_kv[4], X1)
        w_kv[7] = swap(w_kv[6], X1)
        kv_sum = project(w_kv, (0, 1, 2, 4), None, F32)
        w_q[5], w_q[6] = swap(w_q[4], X1), swap(w_q[4], Z1)
        kv = project(w_kv, (3, 5, 6, 7), kv_sum, BF16)
        w_q[3] = swap(w_q[2], X1)
        q_sum = project(w_q, (0, 1, 2, 4), None, F32)
        cut = tokens // 2
        w_q[7] = (swap(w_q[6][:cut], X1), swap(w_q[5][cut:], Z1))

        n_half = chips // ys
        low, high = jnp.concatenate(w_kv[:n_half], 0), jnp.concatenate(w_kv[n_half:], 0)
        w_home = jnp.where(side == 0, low, high)
        w_home_y = swap_y(jnp.where(side == 0, high, low))
        w_home_c = swap(w_home, C1)
        w_home_cy = swap(w_home_y, C1)

        n_cols = GROUP * HEAD_DIM
        states = jax.ShapeDtypeStruct((2, groups, HEAD_DIM, HEAD_DIM), BF16)

        def scan(total, ahead):
            total = total.astype(F32)
            outside = jnp.zeros_like(total)
            for bit, at in ((X1, x), (Z1, z % 2), (Z2, z // 2)):
                got = swap(total.astype(BF16), bit)
                counts = (at == 1) == ahead
                if bit == Z2:
                    return outside, got, counts
                outside = outside + jnp.where(counts, got.astype(F32), 0.0)
                total = total + got.astype(F32)

        totals = jax.ShapeDtypeStruct(states.shape[1:], BF16)
        state, total = kernel_call(state_kernel, out_shape=(states, totals))(kv)
        outside, got, counts = scan(total, True)
        outside = outside + jnp.where(counts, got.astype(F32), 0.0)
        prefix = jnp.stack(
            [
                outside + jnp.where(core == 1, state[1].astype(F32), 0.0),
                outside + jnp.where(core == 0, state[0].astype(F32), 0.0),
            ]
        ).astype(BF16)
        q_spec = pl.BlockSpec((tokens, n_cols), lambda n, g: (n, g))
        gq = kernel_call(
            grad_query_kernel,
            out_shape=jax.ShapeDtypeStruct((2 * tokens, groups * n_cols), BF16),
            grid=(2, groups),
            in_specs=[
                pl.BlockSpec((tokens, HEAD_DIM), lambda n, g: (n, 2 * g)),
                pl.BlockSpec((tokens, HEAD_DIM), lambda n, g: (n, 2 * g + 1)),
                q_spec,
                pl.BlockSpec((1, 1, HEAD_DIM, HEAD_DIM), lambda n, g: (n, g, 0, 0)),
            ],
            out_specs=q_spec,
        )(kv, kv, do_all, prefix)

        def back(which, after=None):
            keep, send = back_call(
                scalar(side), gq, [w_q[i] for i in which], [w_q[i + n_half] for i in which]
            )
            got = swap(send, C1)
            if after is not None:
                keep = gate(keep, after)
            away = (keep[1] + got[1].astype(F32)).astype(BF16)
            return keep, got, swap_y(away), away

        sums = [back((0, 1))]
        sums.append(back((2,), sums[0][3]))
        q_sum = project(w_q, (5, 6), q_sum, F32)
        q, gs, total = project(w_q, (3, 7), q_sum, BF16, do_all)
        outside, got, counts = scan(total, False)
        inner = []
        for g in range(groups):
            inner.append(
                kernel_call(
                    inner_kernel,
                    out_shape=jax.ShapeDtypeStruct((2 * tokens, 2 * HEAD_DIM), F32),
                    grid=(2,),
                    in_specs=[
                        pl.BlockSpec((tokens, n_cols), lambda n, g=g: (n, g)),
                        pl.BlockSpec((tokens, HEAD_DIM), lambda n, g=g: (n, 2 * g)),
                        pl.BlockSpec((tokens, HEAD_DIM), lambda n, g=g: (n, 2 * g + 1)),
                        pl.BlockSpec((tokens, n_cols), lambda n, g=g: (n, g)),
                    ],
                    out_specs=pl.BlockSpec((tokens, 2 * HEAD_DIM), lambda n: (n, 0)),
                )(q, kv, kv, do_all)
            )
        sums.append(back((3,)))
        flags = jnp.stack([counts, core == 0]).astype(jnp.int32)
        part = jax.ShapeDtypeStruct((tokens, 2 * groups * HEAD_DIM), BF16)
        vmem = pl.BlockSpec(memory_space=pltpu.VMEM)
        gkv, gkv_other = kernel_call(
            outer_kernel,
            out_shape=(part, part),
            in_specs=[pl.BlockSpec(memory_space=pltpu.SMEM)] + [vmem] * (4 + groups),
            out_specs=(vmem, vmem),
        )(flags, kv, outside, got, gs, *inner)
        far_other, far = swap_y(gkv_other), swap_y(gkv)
        gkv_c, far_c = swap(gkv_other, C1), swap(far_other, C1)
        slots, width = n_half, sums[0][0].shape[3]
        block, steps = (1, tokens, width), []
        for keep, core_got, far_got, _ in sums:
            last = keep.shape[1] - 1
            for array in (keep, core_got):
                steps.append(
                    (array, (1,) + block, lambda i, last=last: (0, jnp.minimum(i, last), 0, 0))
                )
            steps.append((far_got, block, lambda i, last=last: (jnp.minimum(i, last), 0, 0)))
        home = kernel_call(
            home_kernel,
            out_shape=jax.ShapeDtypeStruct((slots, tokens, width), F32),
            grid=(slots,),
            in_specs=[pl.BlockSpec(gkv.shape, lambda i: (0, 0))] * 2
            + [pl.BlockSpec((width, w_home.shape[1]), lambda i: (i, 0))] * 2
            + [pl.BlockSpec(shape, index) for _, shape, index in steps],
            out_specs=pl.BlockSpec(block, lambda i: (i, 0, 0)),
        )(gkv, gkv_c, w_home, w_home_c, *(array for array, _, _ in steps))
        by_slot = (slots, width, w_home.shape[1])
        w_far = fetch(w_home_y.reshape(by_slot), w_home_cy.reshape(by_slot))
        return kernel_call(
    finish_kernel,
    out_shape=jax.ShapeDtypeStruct((tokens, slots * width), BF16),
    in_specs=[pl.BlockSpec(memory_space=pltpu.SMEM)] + [vmem] * 5,
    out_specs=vmem,
        )(
            scalar(chip % per_half),
            home,
            far,
            far_c,
            *w_far,
        )

    return local


def solution(mesh):
    n_seq, n_head = mesh.shape["seq"], mesh.shape["head"]
    groups = KV_HEADS // n_head
    split = n_seq == 4 * 2 * 2 and groups % 2 == 0 and n_head == 2
    local = make_split(n_seq // 4, 2, n_head) if split else make_plain()

    spec = P("seq", "head")
    return jax.shard_map(local, mesh=mesh, in_specs=(spec,) * 5, out_specs=spec, check_vma=False)
```

```python
import jax
import jax.numpy as jnp
from jax import lax
from jax.experimental import pallas as pl
from jax.experimental.pallas import tpu as pltpu
from jax.sharding import PartitionSpec as P


HEADS = 32
KV_HEADS = 8
HEAD_DIM = 128
GROUP = HEADS // KV_HEADS
FACTOR = HEAD_DIM ** (-0.5)
F32 = jnp.float32
BF16 = jnp.bfloat16


def kernel_call(body, **kwargs):
    return pl.pallas_call(
        body, compiler_params=pltpu.CompilerParams(vmem_limit_bytes=20 * 2**20), **kwargs
    )


def dot_nt(a, b):
    return lax.dot_general(a, b, (((1,), (1,)), ((), ())), preferred_element_type=F32)


def make_plain():
    def local(activations, grad_out, query_weight, key_weight, value_weight):
        gathered = tuple(
            lax.all_gather(w, "seq", axis=0, tiled=True)
            for w in (query_weight, key_weight, value_weight)
        )
        tokens = activations.shape[0]
        whole = lax.all_gather(activations, "head", axis=1, tiled=True)
        queries, keys, values = (
            jnp.dot(whole, w, preferred_element_type=F32).astype(BF16) for w in gathered
        )
        groups = keys.shape[1] // HEAD_DIM
        q = queries.reshape(tokens, groups, GROUP, HEAD_DIM)
        k = keys.reshape(tokens, groups, HEAD_DIM)
        v = values.reshape(tokens, groups, HEAD_DIM)
        do = grad_out.reshape(tokens, groups, GROUP, HEAD_DIM)
        kv_state = jnp.einsum("tgd,tge->gde", k, v, preferred_element_type=F32).astype(BF16)
        grad_state = (
            FACTOR * jnp.einsum("tghd,tghe->gde", q, do, preferred_element_type=F32)
        ).astype(BF16)
        every_kv = lax.all_gather(kv_state[None], "seq", axis=0, tiled=True)
        every_grad = lax.all_gather(grad_state[None], "seq", axis=0, tiled=True)
        position = lax.axis_index("seq")
        order = jnp.arange(every_kv.shape[0], dtype=jnp.int32)
        before = (order < position).astype(BF16)
        after = (order > position).astype(BF16)
        prefix = jnp.einsum("n,ngde->gde", before, every_kv, preferred_element_type=F32).astype(BF16)
        suffix = jnp.einsum("n,ngde->gde", after, every_grad, preferred_element_type=F32).astype(BF16)
        causal = jnp.arange(tokens)[:, None] >= jnp.arange(tokens)[None, :]
        s = jnp.where(
            causal, jnp.einsum("tghd,sgd->ghts", q, k, preferred_element_type=F32), 0.0
        ).astype(BF16)
        ds = jnp.where(
            causal, jnp.einsum("tghe,sge->ghts", do, v, preferred_element_type=F32), 0.0
        ).astype(BF16)
        grad_query = FACTOR * (
            jnp.einsum("ghts,sgd->tghd", ds, k, preferred_element_type=F32)
            + jnp.einsum("tghe,gde->tghd", do, prefix, preferred_element_type=F32)
        )
        grad_key = FACTOR * jnp.einsum(
            "ghts,tghd->sgd", ds, q, preferred_element_type=F32
        ) + jnp.einsum("sge,gde->sgd", v, suffix, preferred_element_type=F32)
        grad_value = FACTOR * jnp.einsum(
            "ghts,tghe->sge", s, do, preferred_element_type=F32
        ) + jnp.einsum("sgd,gde->sge", k, suffix, preferred_element_type=F32)
        parts = (
            dot_nt(g.astype(BF16).reshape(tokens, -1), w)
            for g, w in zip((grad_query, grad_key, grad_value), gathered)
        )
        return lax.psum_scatter(
            sum(parts).astype(BF16), "head", scatter_dimension=1, tiled=True
        )

    return local


def mm(a, b, contract):
    return lax.dot_general(a, b, (contract, ((), ())), preferred_element_type=F32)


NN, NT, TN = ((1,), (0,)), ((1,), (1,)), ((0,), (0,))


def head_cols(h):
    return slice(h * HEAD_DIM, (h + 1) * HEAD_DIM)


def state_kernel(kv_ref, out_ref, total_ref):
    tokens = kv_ref.shape[0] // 2
    for g in range(out_ref.shape[1]):
        total = jnp.zeros(total_ref.shape[1:], F32)
        for n in range(out_ref.shape[0]):
            t = slice(n * tokens, (n + 1) * tokens)
            k, v = kv_ref[t, head_cols(2 * g)], kv_ref[t, head_cols(2 * g + 1)]
            state = mm(k, v, TN).astype(BF16)
            out_ref[n, g] = state
            total = total + state.astype(F32)
        total_ref[g] = total.astype(BF16)


def scores_mask(n):
    return lax.broadcasted_iota(jnp.int32, (n, n), 0) <= lax.broadcasted_iota(
        jnp.int32, (n, n), 1
    )


def grad_query_kernel(k_ref, v_ref, do_ref, prefix_ref, out_ref):
    k, v, prefix = k_ref[...], v_ref[...], prefix_ref[0, 0]
    shape = (k.shape[0], k.shape[0])
    mask = lax.broadcasted_iota(jnp.int32, shape, 0) >= lax.broadcasted_iota(jnp.int32, shape, 1)
    for h in range(GROUP):
        do = do_ref[:, head_cols(h)]
        ds = jnp.where(mask, mm(do, v, NT), 0.0).astype(BF16)
        out_ref[:, head_cols(h)] = (FACTOR * (mm(ds, k, NN) + mm(do, prefix, NT))).astype(BF16)


def inner_kernel(q_ref, k_ref, v_ref, do_ref, out_ref):
    k, v = k_ref[...], v_ref[...]
    mask = scores_mask(k.shape[0])
    gk = jnp.zeros(k.shape, F32)
    gv = jnp.zeros(k.shape, F32)
    for h in range(GROUP):
        q, do = q_ref[:, head_cols(h)], do_ref[:, head_cols(h)]
        ds = jnp.where(mask, mm(v, do, NT), 0.0).astype(BF16)
        s = jnp.where(mask, mm(k, q, NT), 0.0).astype(BF16)
        gk = gk + mm(ds, q, NN)
        gv = gv + mm(s, do, NN)
    out_ref[:, head_cols(0)] = FACTOR * gk
    out_ref[:, head_cols(1)] = FACTOR * gv


def outer_kernel(flag_ref, kv_ref, outside_ref, got_ref, state_ref, *refs):
    inner_refs, out_refs = refs[:-2], refs[-2:]
    tokens = kv_ref.shape[0] // 2
    for g, inner_ref in enumerate(inner_refs):
        behind = outside_ref[g] + jnp.where(flag_ref[0] == 1, got_ref[g].astype(F32), 0.0)
        for n in range(2):
            add = (flag_ref[1] == 1) if n == 0 else (flag_ref[1] == 0)
            suffix = behind + jnp.where(add, state_ref[1 - n, g].astype(F32), 0.0)
            suffix = suffix.astype(BF16)
            t = slice(n * tokens, (n + 1) * tokens)
            k, v = kv_ref[t, head_cols(2 * g)], kv_ref[t, head_cols(2 * g + 1)]
            gk = inner_ref[t, head_cols(0)] + mm(v, suffix, NT)
            gv = inner_ref[t, head_cols(1)] + mm(k, suffix, NN)
            out_refs[n][:, head_cols(2 * g)] = gk.astype(BF16)
            out_refs[n][:, head_cols(2 * g + 1)] = gv.astype(BF16)


def project_call(base, x, weights, total, dtype, do=None):
    slots = sorted(weights)
    pieces = [weights[i] if isinstance(weights[i], tuple) else (weights[i],) for i in slots]
    cols = pieces[0][0].shape[1]
    rows = sum(w.shape[0] for w in pieces[0])
    tokens = x.shape[0] // 2
    width = GROUP * HEAD_DIM if do is not None else rows // 2
    n = len(slots)

    def body(base_ref, *refs):
        xs, rest = refs[:n], list(refs[n:])
        ws = [[rest.pop(0) for _ in piece] for piece in pieces]
        acc = rest.pop(0)[...] if total is not None else None
        do_ref = rest.pop(0) if do is not None else None
        for x_ref, w_refs in zip(xs, ws):
            at = 0
            for w_ref in w_refs:
                part = mm(x_ref[:, at : at + w_ref.shape[0]], w_ref[...], NN)
                acc = part if acc is None else acc + part
                at += w_ref.shape[0]
        acc = acc.astype(dtype)
        rest[0][...] = acc
        if do_ref is not None:
            both = None
            for m in range(2):
                t = slice(m * tokens, (m + 1) * tokens)
                state = None
                for h in range(GROUP):
                    part = mm(acc[t, head_cols(h)], do_ref[t, head_cols(h)], TN)
                    state = part if state is None else state + part
                state = (FACTOR * state).astype(BF16)
                rest[1][m, 0] = state
                state = state.astype(F32)
                both = state if both is None else both + state
            rest[2][0] = both.astype(BF16)

    def x_spec(i):
        return pl.BlockSpec((2 * tokens, rows), lambda j, b: (0, b[0] ^ i))

    tile = pl.BlockSpec((2 * tokens, width), lambda j, b: (0, j))
    args = [x] * n + [w for piece in pieces for w in piece]
    in_specs = [x_spec(i) for i in slots]
    in_specs += [
        pl.BlockSpec((w.shape[0], width), lambda j, b: (0, j)) for piece in pieces for w in piece
    ]
    out_shape, out_specs = [jax.ShapeDtypeStruct((2 * tokens, cols), dtype)], [tile]
    if total is not None:
        args.append(total)
        in_specs.append(tile)
    if do is not None:
        args.append(do)
        in_specs.append(tile)
        one = (cols // width, HEAD_DIM, HEAD_DIM)
        out_shape += [jax.ShapeDtypeStruct((2,) + one, BF16), jax.ShapeDtypeStruct(one, BF16)]
        out_specs += [
            pl.BlockSpec((2, 1, HEAD_DIM, HEAD_DIM), lambda j, b: (0, j, 0, 0)),
            pl.BlockSpec((1, HEAD_DIM, HEAD_DIM), lambda j, b: (j, 0, 0)),
        ]
    out = kernel_call(
        body,
        out_shape=out_shape,
        grid_spec=pltpu.PrefetchScalarGridSpec(
            num_scalar_prefetch=1,
            grid=(cols // width,),
            in_specs=in_specs,
            out_specs=out_specs,
        ),
    )(base, *args)
    return out if do is not None else out[0]


def back_call(side, grads, low, high):
    n = len(low)
    pieces = [w if isinstance(w, tuple) else (w,) for w in low + high]
    rows = sum(w.shape[0] for w in pieces[0])
    inner = grads.shape[1]
    tokens = grads.shape[0] // 2
    half = rows // 2

    def body(side_ref, g_ref, *refs):
        rest, (keep_ref, send_ref) = list(refs[:-2]), refs[-2:]
        first = pl.program_id(0) == 0
        for m, piece in enumerate(pieces):
            w = [rest.pop(0)[...] for _ in piece]
            if len(w) > 1:
                w = jnp.concatenate(w, 0)
                w = jnp.where(first, w[:half], w[half:])
            else:
                w = w[0]
            both = mm(g_ref[...], w, NT)
            where = side_ref[0] if m < n else 1 - side_ref[0]
            keep_ref[where, m % n] = both[:tokens]
            send_ref[where, m % n] = both[tokens:].astype(BF16)

    in_specs = [pl.BlockSpec(grads.shape, lambda j, b: (0, 0))]
    for piece in pieces:
        if len(piece) == 1:
            in_specs.append(pl.BlockSpec((half, inner), lambda j, b: (j, 0)))
        else:
            in_specs += [pl.BlockSpec(w.shape, lambda j, b: (0, 0)) for w in piece]
    out = pl.BlockSpec((2, n, tokens, half), lambda j, b: (0, 0, 0, j))
    shape = (2, n, tokens, rows)
    return kernel_call(
        body,
        out_shape=(jax.ShapeDtypeStruct(shape, F32), jax.ShapeDtypeStruct(shape, BF16)),
        grid_spec=pltpu.PrefetchScalarGridSpec(
            num_scalar_prefetch=1, grid=(2,), in_specs=in_specs, out_specs=(out, out)
        ),
    )(side, grads, *(w for piece in pieces for w in piece))


def add_two(total, g, g_other, w, w_other):
    return total + mm(g, w, NT) + mm(g_other, w_other, NT)


def home_kernel(g_ref, g_other_ref, w_ref, w_other_ref, *refs):
    out_ref, triples = refs[-1], [refs[i : i + 3] for i in range(0, len(refs) - 1, 3)]
    slot = pl.program_id(0)
    total = None
    for n, (keep, core, far) in enumerate(triples):
        part = keep[0, 0] + core[0, 0].astype(F32) + far[0].astype(F32)
        total = part if total is None else jnp.where(slot > n, part, total)
    out_ref[0] = add_two(total, g_ref[...], g_other_ref[...], w_ref[...], w_other_ref[...])


def fetch_kernel(*refs):
    n = (len(refs) - 1) // 2
    sems = refs[-1]
    copies = [pltpu.make_async_copy(refs[i], refs[n + i], sems.at[i]) for i in range(n)]
    for copy in copies:
        copy.start()
    for copy in copies:
        copy.wait()


def fetch(*arrays):
    hbm = pl.BlockSpec(memory_space=pl.ANY)
    vmem = pl.BlockSpec(memory_space=pltpu.VMEM)
    return kernel_call(
        fetch_kernel,
        out_shape=[pltpu.VMEM(a.shape, a.dtype) for a in arrays],
        in_specs=[hbm] * len(arrays),
        out_specs=[vmem] * len(arrays),
        scratch_shapes=[pltpu.SemaphoreType.DMA((len(arrays),))],
    )(*arrays)


def finish_kernel(base_ref, sum_ref, g_ref, g_other_ref, w_ref, w_other_ref, out_ref):
    slots, _, width = sum_ref.shape
    for i in range(slots):
        at = base_ref[0] ^ i
        out_ref[:, i * width : (i + 1) * width] = add_two(
            sum_ref[at], g_ref[...], g_other_ref[...], w_ref[at], w_other_ref[at]
        ).astype(BF16)


def make_split(zs, xs, ys):
    n_seq = zs * xs * 2

    def swap(value, bit):
        return lax.ppermute(value, "seq", [(s, s ^ bit) for s in range(n_seq)])

    def swap_y(value):
        return lax.ppermute(value, "head", [(y, y ^ 1) for y in range(ys)])

    Z1, Z2, X1, C1 = 2 * xs, 4 * xs, 2, 1

    def local(activations, grad_out, query_weight, key_weight, value_weight):
        tokens, _ = activations.shape
        groups = key_weight.shape[1] // HEAD_DIM // 2
        seq = lax.axis_index("seq")
        y = lax.axis_index("head")
        core, x, z = seq % 2, (seq // 2) % xs, seq // (2 * xs)
        chip, chips = seq // 2, n_seq // 2
        per_half = chips // ys
        side = (chip // per_half) ^ y

        def cols(w, which):
            n = w.shape[1] // 2
            return lax.dynamic_slice_in_dim(w, which * n, n, 1)

        def own_and_other(own, other):
            return jnp.concatenate([own, swap(other, C1)], 0)

        def in_order(own, other):
            n = own.shape[0]
            both = jnp.zeros((2 * n, own.shape[1]), own.dtype)
            both = lax.dynamic_update_slice_in_dim(both, own, core * n, 0)
            got = swap(other, C1)
            return lax.dynamic_update_slice_in_dim(both, got, (1 - core) * n, 0)

        def keys_and_values(which):
            k, v = cols(key_weight, which), cols(value_weight, which)
            return jnp.concatenate(
                [w[:, head_cols(g)] for g in range(groups) for w in (k, v)], 1
            )

        def gate(value, *first):
            return lax.optimization_barrier((value,) + first)[0]

        def scalar(value):
            return value.reshape(1).astype(jnp.int32)

        chunk_a = in_order(keys_and_values(core), keys_and_values(1 - core))
        chunk_b = in_order(cols(query_weight, core), cols(query_weight, 1 - core))
        do_all = own_and_other(cols(grad_out, core), cols(grad_out, 1 - core))
        acts = jnp.concatenate([activations, swap_y(activations)], 1)
        acts = gate(own_and_other(acts, acts), do_all)
        base = scalar(side * per_half + chip % per_half)

        def project(weights, which, total, dtype, do=None):
            return project_call(
                base, acts, {i: weights[i] for i in which}, total, dtype, do
            )

        w_kv, w_q = [chunk_a] + [None] * (chips - 1), [chunk_b] + [None] * (chips - 1)
        w_kv[4], w_kv[2] = swap(chunk_a, Z2), swap(chunk_a, Z1)
        w_kv[1] = swap(chunk_a, X1)
        w_q[1] = (swap(chunk_b[:tokens], X1), swap(chunk_b[tokens:], X1))
        w_kv[6] = swap(w_kv[4], Z1)
        w_q[4], w_q[2] = swap(chunk_b, Z2), swap(chunk_b, Z1)
        w_kv[3], w_kv[5] = swap(w_kv[2], X1), swap(w_kv[4], X1)
        w_kv[7] = swap(w_kv[6], X1)
        kv_sum = project(w_kv, (0, 1, 2, 4), None, F32)
        w_q[5], w_q[6] = swap(w_q[4], X1), swap(w_q[4], Z1)
        kv = project(w_kv, (3, 5, 6, 7), kv_sum, BF16)
        w_q[3] = swap(w_q[2], X1)
        q_sum = project(w_q, (0, 1, 2, 4), None, F32)
        cut = tokens // 2
        w_q[7] = (swap(w_q[6][:cut], X1), swap(w_q[5][cut:], Z1))

        n_half = chips // ys
        low, high = jnp.concatenate(w_kv[:n_half], 0), jnp.concatenate(w_kv[n_half:], 0)
        w_home = jnp.where(side == 0, low, high)

        def away_rows(first):
            here = jnp.concatenate(w_kv[first:n_half:2], 0)
            there = jnp.concatenate(w_kv[n_half + first :: 2], 0)
            got = swap_y(jnp.where(side == 0, there, here))
            return got.reshape(n_half // 2, 1, rows, got.shape[1])

        rows = chunk_a.shape[0]
        w_home_y = jnp.concatenate([away_rows(0), away_rows(1)], 1)
        w_home_y = w_home_y.reshape(w_home.shape)
        w_home_c = swap(w_home, C1)
        w_home_cy = swap(w_home_y, C1)

        n_cols = GROUP * HEAD_DIM
        states = jax.ShapeDtypeStruct((2, groups, HEAD_DIM, HEAD_DIM), BF16)

        def scan(total, ahead, after=None):
            total = total.astype(F32)
            outside = jnp.zeros_like(total)
            for bit, at in ((X1, x), (Z1, z % 2), (Z2, z // 2)):
                got = swap(total.astype(BF16), bit)
                if after is not None and bit == Z1:
                    got = gate(got, after)
                counts = (at == 1) == ahead
                if bit == Z2:
                    return outside, got, counts
                outside = outside + jnp.where(counts, got.astype(F32), 0.0)
                total = total + got.astype(F32)

        totals = jax.ShapeDtypeStruct(states.shape[1:], BF16)
        state, total = kernel_call(state_kernel, out_shape=(states, totals))(kv)
        outside, got, counts = scan(total, True)
        outside = outside + jnp.where(counts, got.astype(F32), 0.0)
        prefix = jnp.stack(
            [
                outside + jnp.where(core == 1, state[1].astype(F32), 0.0),
                outside + jnp.where(core == 0, state[0].astype(F32), 0.0),
            ]
        ).astype(BF16)
        q_spec = pl.BlockSpec((tokens, n_cols), lambda n, g: (n, g))
        gq = kernel_call(
            grad_query_kernel,
            out_shape=jax.ShapeDtypeStruct((2 * tokens, groups * n_cols), BF16),
            grid=(2, groups),
            in_specs=[
                pl.BlockSpec((tokens, HEAD_DIM), lambda n, g: (n, 2 * g)),
                pl.BlockSpec((tokens, HEAD_DIM), lambda n, g: (n, 2 * g + 1)),
                q_spec,
                pl.BlockSpec((1, 1, HEAD_DIM, HEAD_DIM), lambda n, g: (n, g, 0, 0)),
            ],
            out_specs=q_spec,
        )(kv, kv, do_all, prefix)

        def back(which, after=None):
            keep, send = back_call(
                scalar(side), gq, [w_q[i] for i in which], [w_q[i + n_half] for i in which]
            )
            got = swap(send, C1)
            if after is not None:
                keep = gate(keep, after)
            away = (keep[1] + got[1].astype(F32)).astype(BF16)
            return keep, got, swap_y(away), away

        sums = [back((0, 1))]
        sums.append(back((2,), sums[0][3]))
        q_sum = project(w_q, (5, 6), q_sum, F32)
        q, gs, total = project(w_q, (3, 7), q_sum, BF16, do_all)
        sums.append(back((3,)))
        outside, got, counts = scan(total, False, sums[2][3])
        inner = []
        for g in range(groups):
            inner.append(
                kernel_call(
                    inner_kernel,
                    out_shape=jax.ShapeDtypeStruct((2 * tokens, 2 * HEAD_DIM), F32),
                    grid=(2,),
                    in_specs=[
                        pl.BlockSpec((tokens, n_cols), lambda n, g=g: (n, g)),
                        pl.BlockSpec((tokens, HEAD_DIM), lambda n, g=g: (n, 2 * g)),
                        pl.BlockSpec((tokens, HEAD_DIM), lambda n, g=g: (n, 2 * g + 1)),
                        pl.BlockSpec((tokens, n_cols), lambda n, g=g: (n, g)),
                    ],
                    out_specs=pl.BlockSpec((tokens, 2 * HEAD_DIM), lambda n: (n, 0)),
                )(q, kv, kv, do_all)
            )
        flags = jnp.stack([counts, core == 0]).astype(jnp.int32)
        part = jax.ShapeDtypeStruct((tokens, 2 * groups * HEAD_DIM), BF16)
        vmem = pl.BlockSpec(memory_space=pltpu.VMEM)
        gkv, gkv_other = kernel_call(
            outer_kernel,
            out_shape=(part, part),
            in_specs=[pl.BlockSpec(memory_space=pltpu.SMEM)] + [vmem] * (4 + groups),
            out_specs=(vmem, vmem),
        )(flags, kv, outside, got, gs, *inner)
        far_other, far = swap_y(gkv_other), swap_y(gkv)
        gkv_c, far_c = swap(gkv_other, C1), swap(far_other, C1)
        slots, width = n_half, sums[0][0].shape[3]
        block, steps = (1, tokens, width), []
        for keep, core_got, far_got, _ in sums:
            last = keep.shape[1] - 1
            for array in (keep, core_got):
                steps.append(
                    (array, (1,) + block, lambda i, last=last: (0, jnp.minimum(i, last), 0, 0))
                )
            steps.append((far_got, block, lambda i, last=last: (jnp.minimum(i, last), 0, 0)))
        home = kernel_call(
            home_kernel,
            out_shape=jax.ShapeDtypeStruct((slots, tokens, width), F32),
            grid=(slots,),
            in_specs=[pl.BlockSpec(gkv.shape, lambda i: (0, 0))] * 2
            + [pl.BlockSpec((width, w_home.shape[1]), lambda i: (i, 0))] * 2
            + [pl.BlockSpec(shape, index) for _, shape, index in steps],
            out_specs=pl.BlockSpec(block, lambda i: (i, 0, 0)),
        )(gkv, gkv_c, w_home, w_home_c, *(array for array, _, _ in steps))
        by_slot = (slots, width, w_home.shape[1])
        w_far = fetch(w_home_y.reshape(by_slot), w_home_cy.reshape(by_slot))
        return kernel_call(
    finish_kernel,
    out_shape=jax.ShapeDtypeStruct((tokens, slots * width), BF16),
    in_specs=[pl.BlockSpec(memory_space=pltpu.SMEM)] + [vmem] * 5,
    out_specs=vmem,
        )(
            scalar(chip % per_half),
            home,
            far,
            far_c,
            *w_far,
        )

    return local


def solution(mesh):
    n_seq, n_head = mesh.shape["seq"], mesh.shape["head"]
    groups = KV_HEADS // n_head
    split = n_seq == 4 * 2 * 2 and groups % 2 == 0 and n_head == 2
    local = make_split(n_seq // 4, 2, n_head) if split else make_plain()

    spec = P("seq", "head")
    return jax.shard_map(local, mesh=mesh, in_specs=(spec,) * 5, out_specs=spec, check_vma=False)
```
